32 devices in a mesh: slab: 32 (over z, y, x, core).
Axes of the slice: x: 2, y: 2, z: 4, core: 2. Of those that a mesh axis runs over, the one named last changes fastest.
Arguments:
- points: float32 [4, 128, 128, 64], P(None, 'slab'), may hold values from -6 to 6
- offsets_x: int32 [256], replicated, may hold values from 0 to 124, as said below
- coeffs_x: float32 [4, 256], replicated, may hold values from 0.1 to 1
- offsets_y: int32 [256], replicated, may hold values from 0 to 124, as said below
- coeffs_y: float32 [4, 256], replicated, may hold values from 0.1 to 1
- offsets_z: int32 [128], replicated, may hold values from 0 to 60, as said below
- coeffs_z: float32 [4, 128], replicated, may hold values from 0.1 to 1
Outputs:
- refined: float32 [4, 256, 256, 128], P(None, None, 'slab')
The draws below stay inside these ranges and needn't reach their ends.
Inputs may be any that keep to these rules, and one draw needn't show every extreme that they name: offsets_x[i] lies between i // 2 - 2 and i // 2, clipped to 0 .. 124. offsets_y[i] lies between i // 2 - 2 and i // 2, clipped to 0 .. 124. offsets_z[i] lies between i // 2 - 2 and i // 2, clipped to 0 .. 60.
All inputs are finite; a program needn't handle non-finite values.
Results may differ from the reference program's by a relative error of at most 0.000073.
Values sent between devices are 32-bit elements; how exact they have to be, the bound alone decides.
A program may use at most 64 MiB of HBM per device.

```python
import math
import jax
import jax.numpy as jnp

NY = 128
NZ = 64
NX = 128
MX = 256
MY = 256
MZ = 128


def band_offsets(key, count):
    rows = jnp.arange(2 * count, dtype=jnp.int32)
    jitter = jax.random.randint(key, (2 * count,), 0, 3, dtype=jnp.int32)
    return jnp.clip(rows // 2 - 2 + jitter, 0, count - 4).astype(jnp.int32)


def draw_offsets_x(key, part):
    return band_offsets(jax.random.fold_in(key, 11), NX)


def draw_offsets_y(key, part):
    return band_offsets(jax.random.fold_in(key, 12), NY)


def draw_offsets_z(key, part):
    return band_offsets(jax.random.fold_in(key, 13), NZ)


def steps_of(rng, dims, split, least, largest):
    gain = 1.0
    for dim, shards_of in split:
        steps = jax.random.uniform(jax.random.fold_in(jax.random.fold_in(rng, 6), dim), (shards_of,), jnp.float32, least / len(split), largest / len(split))
        gain = gain * jnp.repeat(jnp.exp(steps), dims[dim] // shards_of).reshape((-1,) + (1,) * (len(dims) - 1 - dim))
    return gain


def normal_values(own_key, extent, spread, reach, pieces=(), kind=jnp.bfloat16):
    entries = spread * jax.random.normal(own_key, extent, jnp.float32)
    if pieces:
        entries = entries * steps_of(own_key, extent, pieces, -0.22, 0.18)
    return jnp.clip(entries, -reach, reach).astype(kind)


def setup_inputs(seed: int = 0) -> dict:
    keys = jax.random.split(jax.random.key(seed), 8)
    points = normal_values(keys[0], (4, NX, NY, NZ), 1.0, 6.0, ((1, 32),), jnp.float32)
    offsets_x = draw_offsets_x(jax.random.fold_in(keys[7], 71), 0)
    coeffs_x = jnp.clip(jnp.exp(jax.random.uniform(keys[2], (4, MX), jnp.float32, math.log(0.1), math.log(1.0))), 0.1, 1.0)
    offsets_y = draw_offsets_y(jax.random.fold_in(keys[7], 71), 0)
    coeffs_y = jnp.clip(jnp.exp(jax.random.uniform(keys[4], (4, MY), jnp.float32, math.log(0.1), math.log(1.0))), 0.1, 1.0)
    offsets_z = draw_offsets_z(jax.random.fold_in(keys[7], 71), 0)
    coeffs_z = jnp.clip(jnp.exp(jax.random.uniform(keys[6], (4, MZ), jnp.float32, math.log(0.1), math.log(1.0))), 0.1, 1.0)
    return {"points": points, "offsets_x": offsets_x, "coeffs_x": coeffs_x, "offsets_y": offsets_y, "coeffs_y": coeffs_y, "offsets_z": offsets_z, "coeffs_z": coeffs_z}


def refine(grid, offsets, coeffs, axis):
    weights = coeffs / jnp.sum(coeffs, axis=0, keepdims=True)
    shape = [1] * grid.ndim
    shape[axis] = -1
    total = None
    for k in range(4):
        picked = jnp.take(grid, (offsets + k).astype(jnp.int32), axis=axis)
        term = picked * weights[k].reshape(shape)
        total = term if total is None else total + term
    return total


def reference(points, offsets_x, coeffs_x, offsets_y, coeffs_y, offsets_z, coeffs_z):
    grid = refine(points, offsets_z, coeffs_z, 3)
    grid = refine(grid, offsets_y, coeffs_y, 2)
    return refine(grid, offsets_x, coeffs_x, 1)
```

```python
import functools

import jax
import jax.numpy as jnp
from jax import lax
from jax.experimental import pallas as pl
from jax.experimental.pallas import tpu as pltpu
from jax.sharding import PartitionSpec as P

MESH = pl.DeviceIdType.MESH
BAND = 4
REACH = BAND + 1
SPAN = BAND + 2


def flip(a, k, chips):
    out = 0
    bit = 1
    while bit < chips:
        a_bit, k_bit = (a // bit) % 2, (k // bit) % 2
        out = out + (a_bit + k_bit - 2 * a_bit * k_bit) * bit
        bit *= 2
    return out


def exchange(
    dims,
    points_ref, oy_ref, cy_ref, oz_ref, cz_ref, cx_ref,
    grid_ref, wx_ref,
    send, direct, passed, wy, rz, rz_lo, mixed,
    send_sem, recv_sem, pass_send_sem, pass_recv_sem,
):
    n, comps, xl, ny, nz, jl, mz = dims
    chips = n // 2
    pairs, lanes = points_ref.shape[0], points_ref.shape[1]
    fold = lanes // nz
    cl = jl // 2
    wide, narrow = 2 * cl + REACH, cl + REACH
    me = lax.axis_index("slab")
    chip, core = me // 2, me % 2
    partner = chip * 2 + 1 - core

    def wide_base(c):
        return jnp.clip(c * 2 * cl - 2, 0, ny - wide)

    def narrow_base(d):
        return jnp.clip(d * cl - 2, 0, ny - narrow)

    def span_base(j):
        return jnp.clip((me * jl + j) // 2 - 2, 0, ny - SPAN)

    rows_of_y = send.reshape(ny, pairs, lanes)

    barrier = pltpu.get_barrier_semaphore()
    pl.semaphore_signal(barrier, inc=1, device_id=(partner,), device_id_type=MESH)

    @pl.loop(1, chips)
    def _(k):
        other = flip(chip, k, chips) * 2 + core
        pl.semaphore_signal(barrier, inc=1, device_id=(other,), device_id_type=MESH)

    for p in range(pairs):
        send[pl.ds(p, ny, stride=pairs), :] = points_ref[p].T

    pl.semaphore_wait(barrier, chips)

    def out_copy(k):
        target = flip(chip, k, chips)
        return pltpu.make_async_remote_copy(
            src_ref=rows_of_y.at[pl.ds(wide_base(target), wide)],
            dst_ref=direct.at[k],
            send_sem=send_sem.at[k],
            recv_sem=recv_sem.at[k],
            device_id=(target * 2 + core,),
            device_id_type=MESH,
        )

    def pass_copy(k):
        skip = narrow_base(partner) - wide_base(chip)
        return pltpu.make_async_remote_copy(
            src_ref=direct.at[k, pl.ds(skip, narrow)],
            dst_ref=passed.at[k],
            send_sem=pass_send_sem.at[k],
            recv_sem=pass_recv_sem.at[k],
            device_id=(partner,),
            device_id_type=MESH,
        )

    @pl.loop(1, chips)
    def _(k):
        out_copy(k).start()

    own = pl.ds(wide_base(chip), wide)
    stay = pltpu.make_async_copy(rows_of_y.at[own], direct.at[0], recv_sem.at[0])
    stay.start()

    wx_ref[...] = cx_ref[...] / jnp.sum(cx_ref[...], axis=0, keepdims=True)
    wz = cz_ref[...] / jnp.sum(cz_ref[...], axis=0, keepdims=True)
    at = lax.broadcasted_iota(jnp.int32, (nz, mz), 0)
    first = jnp.broadcast_to(oz_ref[...], (nz, mz))
    band = jnp.zeros((nz, mz), jnp.float32)
    for k in range(BAND):
        band = band + jnp.where(at == first + k, jnp.broadcast_to(wz[k : k + 1], (nz, mz)), 0.0)
    high = band.astype(jnp.bfloat16)
    low = (band - high.astype(jnp.float32)).astype(jnp.bfloat16)
    rz[...] = jnp.zeros_like(rz)
    rz_lo[...] = jnp.zeros_like(rz_lo)
    for f in range(fold):
        rz[f * nz : (f + 1) * nz, f * mz : (f + 1) * mz] = high
        rz[lanes + f * nz : lanes + (f + 1) * nz, f * mz : (f + 1) * mz] = high
        rz_lo[f * nz : (f + 1) * nz, f * mz : (f + 1) * mz] = low
    for j in range(jl):
        coeffs = [jnp.full((pairs, lanes), cy_ref[k, me * jl + j]) for k in range(BAND)]
        total = coeffs[0] + coeffs[1] + coeffs[2] + coeffs[3]
        coeffs = [c / total for c in coeffs]
        skip = jnp.full((pairs, lanes), oy_ref[me * jl + j] - span_base(j))
        for m in range(SPAN):
            weight = jnp.zeros((pairs, lanes), jnp.float32)
            for k in range(max(0, m - SPAN + BAND), min(BAND, m + 1)):
                weight = jnp.where(skip == m - k, coeffs[k], weight)
            wy[j * SPAN + m] = weight

    def refine_y(place, load, base):
        for j in range(jl):
            row = span_base(j) - base
            acc = wy[j * SPAN] * load(row)
            for m in range(1, SPAN):
                acc = acc + wy[j * SPAN + m] * load(row + m)
            mixed[pl.ds(place * pairs * jl + j, pairs, stride=jl), :] = acc

    def refine_z(devices):
        rows = pairs * jl * len(devices)
        x = mixed[:rows]
        hi = x.astype(jnp.bfloat16)
        lo = (x - hi.astype(jnp.float32)).astype(jnp.bfloat16)
        both = jnp.concatenate([hi, lo], axis=1)
        res = jnp.dot(both, rz[...], preferred_element_type=jnp.float32)
        res = res + jnp.dot(hi, rz_lo[...], preferred_element_type=jnp.float32)
        per = pairs // comps
        for q, device in enumerate(devices):
            for p in range(pairs):
                for f in range(fold):
                    spot = (p // per, device * xl + (p % per) * fold + f)
                    top = (q * pairs + p) * jl
                    grid_ref[spot] = res[top : top + jl, f * mz : (f + 1) * mz]

    def from_direct(place, k):
        refine_y(
            place,
            lambda row: direct[k, row],
            wide_base(chip),
        )
        return flip(chip, k, chips) * 2 + core

    def from_passed(place, k):
        refine_y(
            place,
            lambda row: passed[k, row],
            narrow_base(me),
        )
        return flip(chip, k, chips) * 2 + 1 - core

    stay.wait()
    pass_copy(0).start()
    refine_z([from_direct(0, 0)])

    @pl.loop(1, chips)
    def _(k):
        out_copy(k).wait_recv()
        pass_copy(k).start()
        one = from_direct(0, k)
        pass_copy(k - 1).wait_recv()
        two = from_passed(1, k - 1)
        refine_z([one, two])

    pass_copy(chips - 1).wait_recv()
    refine_z([from_passed(0, chips - 1)])

    @pl.loop(1, chips)
    def _(k):
        out_copy(k).wait_send()

    @pl.loop(0, chips)
    def _(k):
        pass_copy(k).wait_send()


def refine_x(rows, ox_ref, wx_ref, grid_ref, out_ref):
    comps = grid_ref.shape[0]
    start = pl.program_id(0) * rows

    @pl.loop(0, rows, unroll=4)
    def _(r):
        i = start + r
        first = ox_ref[i]
        weights = [wx_ref[k, i] for k in range(BAND)]
        for c in range(comps):
            acc = weights[0] * grid_ref[c, first]
            for k in range(1, BAND):
                acc = acc + weights[k] * grid_ref[c, first + k]
            out_ref[c, r] = acc


def solution(mesh):
    n = mesh.shape["slab"]
    vmem = pl.BlockSpec(memory_space=pltpu.VMEM)
    smem = pl.BlockSpec(memory_space=pltpu.SMEM)

    def body(points, offsets_x, coeffs_x, offsets_y, coeffs_y, offsets_z, coeffs_z):
        comps, xl, ny, nz = points.shape
        nx = xl * n
        mx, my, mz = offsets_x.shape[0], offsets_y.shape[0], offsets_z.shape[0]
        jl = my // n
        fold = 128 // nz
        pairs = comps * xl // fold
        lanes = fold * nz
        chips = n // 2
        cl = jl // 2
        wide, narrow = 2 * cl + REACH, cl + REACH
        slab = jnp.transpose(points, (0, 1, 3, 2)).reshape(pairs, lanes, ny)
        f32, bf16 = jnp.float32, jnp.bfloat16
        grid, wx = pl.pallas_call(
            functools.partial(exchange, (n, comps, xl, ny, nz, jl, mz)),
            out_shape=(
                jax.ShapeDtypeStruct((comps, nx, jl, mz), f32),
                jax.ShapeDtypeStruct((BAND, mx), f32),
            ),
            in_specs=[vmem, smem, smem, vmem, vmem, vmem],
            out_specs=(vmem, vmem),
            scratch_shapes=[
                pltpu.VMEM((ny * pairs, lanes), f32),
                pltpu.VMEM((chips, wide, pairs, lanes), f32),
                pltpu.VMEM((chips, narrow, pairs, lanes), f32),
                pltpu.VMEM((jl * SPAN, pairs, lanes), f32),
                pltpu.VMEM((2 * lanes, fold * mz), bf16),
                pltpu.VMEM((lanes, fold * mz), bf16),
                pltpu.VMEM((2 * pairs * jl, lanes), f32),
                pltpu.SemaphoreType.DMA((chips,)),
                pltpu.SemaphoreType.DMA((chips,)),
                pltpu.SemaphoreType.DMA((chips,)),
                pltpu.SemaphoreType.DMA((chips,)),
            ],
            compiler_params=pltpu.CompilerParams(collective_id=0, has_side_effects=True),
            name="exchange",
        )(slab, offsets_y, coeffs_y, offsets_z.reshape(1, mz), coeffs_z, coeffs_x)
        steps = 8
        rows = mx // steps
        return pl.pallas_call(
            functools.partial(refine_x, rows),
            out_shape=jax.ShapeDtypeStruct((comps, mx, jl, mz), f32),
            grid=(steps,),
            in_specs=[smem, smem, pl.BlockSpec((comps, nx, jl, mz), lambda s: (0, 0, 0, 0))],
            out_specs=pl.BlockSpec((comps, rows, jl, mz), lambda s: (0, s, 0, 0)),
            name="refine_x",
        )(offsets_x, wx, grid)

    return jax.shard_map(
        body,
        mesh=mesh,
        in_specs=(P(None, "slab", None, None), P(), P(), P(), P(), P(), P()),
        out_specs=P(None, None, "slab", None),
        check_vma=False,
    )
```

```python
import functools

import jax
import jax.numpy as jnp
from jax import lax
from jax.experimental import pallas as pl
from jax.experimental.pallas import tpu as pltpu
from jax.sharding import PartitionSpec as P

MESH = pl.DeviceIdType.MESH
BAND = 4
REACH = BAND + 1
SPAN = BAND + 2


def flip(a, k, chips):
    out = 0
    bit = 1
    while bit < chips:
        a_bit, k_bit = (a // bit) % 2, (k // bit) % 2
        out = out + (a_bit + k_bit - 2 * a_bit * k_bit) * bit
        bit *= 2
    return out


def exchange(
    dims,
    points_ref, oy_ref, cy_ref, oz_ref, cz_ref, cx_ref,
    grid_ref, wx_ref,
    send, direct, passed, wy, rz, rz_lo, mixed,
    send_sem, recv_sem, pass_send_sem, pass_recv_sem,
):
    n, comps, xl, ny, nz, jl, mz = dims
    chips = n // 2
    pairs, lanes = points_ref.shape[0], points_ref.shape[1]
    fold = lanes // nz
    cl = jl // 2
    wide, narrow = 2 * cl + REACH, cl + REACH
    me = lax.axis_index("slab")
    chip, core = me // 2, me % 2
    partner = chip * 2 + 1 - core

    def wide_base(c):
        return jnp.clip(c * 2 * cl - 2, 0, ny - wide)

    def narrow_base(d):
        return jnp.clip(d * cl - 2, 0, ny - narrow)

    def span_base(j):
        return jnp.clip((me * jl + j) // 2 - 2, 0, ny - SPAN)

    rows_of_y = send.reshape(ny, pairs, lanes)

    barrier = pltpu.get_barrier_semaphore()
    pl.semaphore_signal(barrier, inc=1, device_id=(partner,), device_id_type=MESH)

    @pl.loop(1, chips)
    def _(k):
        other = flip(chip, k, chips) * 2 + core
        pl.semaphore_signal(barrier, inc=1, device_id=(other,), device_id_type=MESH)

    for p in range(pairs):
        send[pl.ds(p, ny, stride=pairs), :] = points_ref[p].T

    pl.semaphore_wait(barrier, chips)

    def out_copy(k):
        target = flip(chip, k, chips)
        return pltpu.make_async_remote_copy(
            src_ref=rows_of_y.at[pl.ds(wide_base(target), wide)],
            dst_ref=direct.at[k],
            send_sem=send_sem.at[k],
            recv_sem=recv_sem.at[k],
            device_id=(target * 2 + core,),
            device_id_type=MESH,
        )

    def pass_copy(k):
        skip = narrow_base(partner) - wide_base(chip)
        return pltpu.make_async_remote_copy(
            src_ref=direct.at[k, pl.ds(skip, narrow)],
            dst_ref=passed.at[k],
            send_sem=pass_send_sem.at[k],
            recv_sem=pass_recv_sem.at[k],
            device_id=(partner,),
            device_id_type=MESH,
        )

    @pl.loop(1, chips)
    def _(k):
        out_copy(k).start()

    own = pl.ds(wide_base(chip), wide)
    stay = pltpu.make_async_copy(rows_of_y.at[own], direct.at[0], recv_sem.at[0])
    stay.start()

    wx_ref[...] = cx_ref[...] / jnp.sum(cx_ref[...], axis=0, keepdims=True)
    wz = cz_ref[...] / jnp.sum(cz_ref[...], axis=0, keepdims=True)
    at = lax.broadcasted_iota(jnp.int32, (nz, mz), 0)
    first = jnp.broadcast_to(oz_ref[...], (nz, mz))
    band = jnp.zeros((nz, mz), jnp.float32)
    for k in range(BAND):
        band = band + jnp.where(at == first + k, jnp.broadcast_to(wz[k : k + 1], (nz, mz)), 0.0)
    high = band.astype(jnp.bfloat16)
    low = (band - high.astype(jnp.float32)).astype(jnp.bfloat16)
    rz[...] = jnp.zeros_like(rz)
    rz_lo[...] = jnp.zeros_like(rz_lo)
    for f in range(fold):
        rz[f * nz : (f + 1) * nz, f * mz : (f + 1) * mz] = high
        rz[lanes + f * nz : lanes + (f + 1) * nz, f * mz : (f + 1) * mz] = high
        rz_lo[f * nz : (f + 1) * nz, f * mz : (f + 1) * mz] = low
    for j in range(jl):
        coeffs = [jnp.full((pairs, lanes), cy_ref[k, me * jl + j]) for k in range(BAND)]
        total = coeffs[0] + coeffs[1] + coeffs[2] + coeffs[3]
        coeffs = [c / total for c in coeffs]
        skip = jnp.full((pairs, lanes), oy_ref[me * jl + j] - span_base(j))
        for m in range(SPAN):
            weight = jnp.zeros((pairs, lanes), jnp.float32)
            for k in range(max(0, m - SPAN + BAND), min(BAND, m + 1)):
                weight = jnp.where(skip == m - k, coeffs[k], weight)
            wy[j * SPAN + m] = weight

    def refine_y(place, load, base):
        for j in range(jl):
            row = span_base(j) - base
            acc = wy[j * SPAN] * load(row)
            for m in range(1, SPAN):
                acc = acc + wy[j * SPAN + m] * load(row + m)
            mixed[pl.ds(place * pairs * jl + j, pairs, stride=jl), :] = acc

    def refine_z(devices):
        rows = pairs * jl * len(devices)
        x = mixed[:rows]
        hi = x.astype(jnp.bfloat16)
        lo = (x - hi.astype(jnp.float32)).astype(jnp.bfloat16)
        both = jnp.concatenate([hi, lo], axis=1)
        res = jnp.dot(both, rz[...], preferred_element_type=jnp.float32)
        res = res + jnp.dot(hi, rz_lo[...], preferred_element_type=jnp.float32)
        per = pairs // comps
        for q, device in enumerate(devices):
            for p in range(pairs):
                for f in range(fold):
                    spot = (p // per, device * xl + (p % per) * fold + f)
                    top = (q * pairs + p) * jl
                    grid_ref[spot] = res[top : top + jl, f * mz : (f + 1) * mz]

    def from_direct(place, k):
        refine_y(
            place,
            lambda row: direct[k, row],
            wide_base(chip),
        )
        return flip(chip, k, chips) * 2 + core

    def from_passed(place, k):
        refine_y(
            place,
            lambda row: passed[k, row],
            narrow_base(me),
        )
        return flip(chip, k, chips) * 2 + 1 - core

    stay.wait()
    pass_copy(0).start()
    refine_z([from_direct(0, 0)])

    @pl.loop(1, chips)
    def _(k):
        out_copy(k).wait_recv()
        pass_copy(k).start()
        one = from_direct(0, k)
        pass_copy(k - 1).wait_recv()
        two = from_passed(1, k - 1)
        refine_z([one, two])

    pass_copy(chips - 1).wait_recv()
    refine_z([from_passed(0, chips - 1)])

    @pl.loop(1, chips)
    def _(k):
        out_copy(k).wait_send()

    @pl.loop(0, chips)
    def _(k):
        pass_copy(k).wait_send()


def refine_x(rows, ox_ref, wx_ref, grid_ref, out_ref):
    comps = grid_ref.shape[0]
    start = pl.program_id(0) * rows

    @pl.loop(0, rows, unroll=4)
    def _(r):
        i = start + r
        first = ox_ref[i]
        weights = [wx_ref[k, i] for k in range(BAND)]
        for c in range(comps):
            acc = weights[0] * grid_ref[c, first]
            for k in range(1, BAND):
                acc = acc + weights[k] * grid_ref[c, first + k]
            out_ref[c, r] = acc


def solution(mesh):
    n = mesh.shape["slab"]
    vmem = pl.BlockSpec(memory_space=pltpu.VMEM)
    smem = pl.BlockSpec(memory_space=pltpu.SMEM)

    def body(points, offsets_x, coeffs_x, offsets_y, coeffs_y, offsets_z, coeffs_z):
        comps, xl, ny, nz = points.shape
        nx = xl * n
        mx, my, mz = offsets_x.shape[0], offsets_y.shape[0], offsets_z.shape[0]
        jl = my // n
        fold = 128 // nz
        pairs = comps * xl // fold
        lanes = fold * nz
        chips = n // 2
        cl = jl // 2
        wide, narrow = 2 * cl + REACH, cl + REACH
        slab = jnp.transpose(points, (0, 1, 3, 2)).reshape(pairs, lanes, ny)
        f32, bf16 = jnp.float32, jnp.bfloat16
        grid, wx = pl.pallas_call(
            functools.partial(exchange, (n, comps, xl, ny, nz, jl, mz)),
            out_shape=(
                pltpu.VMEM((comps, nx, jl, mz), f32),
                jax.ShapeDtypeStruct((BAND, mx), f32),
            ),
            in_specs=[vmem, smem, smem, vmem, vmem, vmem],
            out_specs=(vmem, vmem),
            scratch_shapes=[
                pltpu.VMEM((ny * pairs, lanes), f32),
                pltpu.VMEM((chips, wide, pairs, lanes), f32),
                pltpu.VMEM((chips, narrow, pairs, lanes), f32),
                pltpu.VMEM((jl * SPAN, pairs, lanes), f32),
                pltpu.VMEM((2 * lanes, fold * mz), bf16),
                pltpu.VMEM((lanes, fold * mz), bf16),
                pltpu.VMEM((2 * pairs * jl, lanes), f32),
                pltpu.SemaphoreType.DMA((chips,)),
                pltpu.SemaphoreType.DMA((chips,)),
                pltpu.SemaphoreType.DMA((chips,)),
                pltpu.SemaphoreType.DMA((chips,)),
            ],
            compiler_params=pltpu.CompilerParams(collective_id=0, has_side_effects=True),
            name="exchange",
        )(slab, offsets_y, coeffs_y, offsets_z.reshape(1, mz), coeffs_z, coeffs_x)
        steps = 8
        rows = mx // steps
        return pl.pallas_call(
            functools.partial(refine_x, rows),
            out_shape=jax.ShapeDtypeStruct((comps, mx, jl, mz), f32),
            grid=(steps,),
            in_specs=[smem, smem, vmem],
            out_specs=pl.BlockSpec((comps, rows, jl, mz), lambda s: (0, s, 0, 0)),
            name="refine_x",
        )(offsets_x, wx, pltpu.with_memory_space_constraint(grid, pltpu.VMEM))

    return jax.shard_map(
        body,
        mesh=mesh,
        in_specs=(P(None, "slab", None, None), P(), P(), P(), P(), P(), P()),
        out_specs=P(None, None, "slab", None),
        check_vma=False,
    )
```

```python
import functools

import jax
import jax.numpy as jnp
from jax import lax
from jax.experimental import pallas as pl
from jax.experimental.pallas import tpu as pltpu
from jax.sharding import PartitionSpec as P

MESH = pl.DeviceIdType.MESH
BAND = 4
REACH = BAND + 1
SPAN = BAND + 2
BELOW, ABOVE = 2, 3
PLANES = 4


def flip(a, k, chips):
    out = 0
    bit = 1
    while bit < chips:
        a_bit, k_bit = (a // bit) % 2, (k // bit) % 2
        out = out + (a_bit + k_bit - 2 * a_bit * k_bit) * bit
        bit *= 2
    return out


def span_of(me, jl, ny, j):
    return jnp.clip((me * jl + j) // 2 - 2, 0, ny - SPAN)


def make_weights(dims, me, span_base, oy_ref, cy_ref, oz_ref, cz_ref, cx_ref, wx_ref, wy, rz, rz_lo):
    n, comps, xl, ny, nz, jl, mz = dims
    pairs, lanes = wy.shape[1], wy.shape[2]
    fold = lanes // nz
    wx_ref[...] = cx_ref[...] / jnp.sum(cx_ref[...], axis=0, keepdims=True)
    wz = cz_ref[...] / jnp.sum(cz_ref[...], axis=0, keepdims=True)
    at = lax.broadcasted_iota(jnp.int32, (nz, mz), 0)
    first = jnp.broadcast_to(oz_ref[...], (nz, mz))
    band = jnp.zeros((nz, mz), jnp.float32)
    for k in range(BAND):
        band = band + jnp.where(at == first + k, jnp.broadcast_to(wz[k : k + 1], (nz, mz)), 0.0)
    high = band.astype(jnp.bfloat16)
    low = (band - high.astype(jnp.float32)).astype(jnp.bfloat16)
    rz[...] = jnp.zeros_like(rz)
    rz_lo[...] = jnp.zeros_like(rz_lo)
    for f in range(fold):
        rz[f * nz : (f + 1) * nz, f * mz : (f + 1) * mz] = high
        rz[lanes + f * nz : lanes + (f + 1) * nz, f * mz : (f + 1) * mz] = high
        rz_lo[f * nz : (f + 1) * nz, f * mz : (f + 1) * mz] = low
    for j in range(jl):
        coeffs = [jnp.full((pairs, lanes), cy_ref[k, me * jl + j]) for k in range(BAND)]
        total = coeffs[0] + coeffs[1] + coeffs[2] + coeffs[3]
        coeffs = [c / total for c in coeffs]
        skip = jnp.full((pairs, lanes), oy_ref[me * jl + j] - span_base(j))
        for m in range(SPAN):
            weight = jnp.zeros((pairs, lanes), jnp.float32)
            for k in range(max(0, m - SPAN + BAND), min(BAND, m + 1)):
                weight = jnp.where(skip == m - k, coeffs[k], weight)
            wy[j * SPAN + m] = weight


def refine_y(jl, pairs, span_base, wy, mixed, place, load, base):
    for j in range(jl):
        row = span_base(j) - base
        acc = wy[j * SPAN] * load(row)
        for m in range(1, SPAN):
            acc = acc + wy[j * SPAN + m] * load(row + m)
        mixed[pl.ds(place * pairs * jl + j, pairs, stride=jl), :] = acc


def refine_z(dims, pairs, mixed, rz, rz_lo, grid_ref, devices):
    n, comps, xl, ny, nz, jl, mz = dims
    fold = mixed.shape[1] // nz
    rows = pairs * jl * len(devices)
    x = mixed[:rows]
    hi = x.astype(jnp.bfloat16)
    lo = (x - hi.astype(jnp.float32)).astype(jnp.bfloat16)
    both = jnp.concatenate([hi, lo], axis=1)
    res = jnp.dot(both, rz[...], preferred_element_type=jnp.float32)
    res = res + jnp.dot(hi, rz_lo[...], preferred_element_type=jnp.float32)
    per = pairs // comps
    for q, device in enumerate(devices):
        for p in range(pairs):
            for f in range(fold):
                spot = (p // per, device * xl + (p % per) * fold + f)
                top = (q * pairs + p) * jl
                grid_ref[spot] = res[top : top + jl, f * mz : (f + 1) * mz]


def exchange(
    dims,
    points_ref, oy_ref, cy_ref, oz_ref, cz_ref, cx_ref,
    grid_ref, wx_ref,
    send, direct, passed, wy, rz, rz_lo, mixed,
    send_sem, recv_sem, pass_send_sem, pass_recv_sem,
):
    n, comps, xl, ny, nz, jl, mz = dims
    chips = n // 2
    pairs, lanes = points_ref.shape[0], points_ref.shape[1]
    cl = jl // 2
    wide, narrow = 2 * cl + REACH, cl + REACH
    me = lax.axis_index("slab")
    chip, core = me // 2, me % 2
    partner = chip * 2 + 1 - core

    def wide_base(c):
        return jnp.clip(c * 2 * cl - 2, 0, ny - wide)

    def narrow_base(d):
        return jnp.clip(d * cl - 2, 0, ny - narrow)

    span_base = functools.partial(span_of, me, jl, ny)

    rows_of_y = send.reshape(ny, pairs, lanes)

    barrier = pltpu.get_barrier_semaphore()
    pl.semaphore_signal(barrier, inc=1, device_id=(partner,), device_id_type=MESH)

    @pl.loop(1, chips)
    def _(k):
        other = flip(chip, k, chips) * 2 + core
        pl.semaphore_signal(barrier, inc=1, device_id=(other,), device_id_type=MESH)

    for p in range(pairs):
        send[pl.ds(p, ny, stride=pairs), :] = points_ref[p].T

    pl.semaphore_wait(barrier, chips)

    def out_copy(k):
        target = flip(chip, k, chips)
        return pltpu.make_async_remote_copy(
            src_ref=rows_of_y.at[pl.ds(wide_base(target), wide)],
            dst_ref=direct.at[k],
            send_sem=send_sem.at[k],
            recv_sem=recv_sem.at[k],
            device_id=(target * 2 + core,),
            device_id_type=MESH,
        )

    def pass_copy(k):
        skip = narrow_base(partner) - wide_base(chip)
        return pltpu.make_async_remote_copy(
            src_ref=direct.at[k, pl.ds(skip, narrow)],
            dst_ref=passed.at[k],
            send_sem=pass_send_sem.at[k],
            recv_sem=pass_recv_sem.at[k],
            device_id=(partner,),
            device_id_type=MESH,
        )

    @pl.loop(1, chips)
    def _(k):
        out_copy(k).start()

    own = pl.ds(wide_base(chip), wide)
    stay = pltpu.make_async_copy(rows_of_y.at[own], direct.at[0], recv_sem.at[0])
    stay.start()

    make_weights(dims, me, span_base, oy_ref, cy_ref, oz_ref, cz_ref, cx_ref, wx_ref, wy, rz, rz_lo)

    def from_direct(place, k):
        refine_y(
            jl, pairs, span_base, wy, mixed, place,
            lambda row: direct[k, row],
            wide_base(chip),
        )
        return flip(chip, k, chips) * 2 + core

    def from_passed(place, k):
        refine_y(
            jl, pairs, span_base, wy, mixed, place,
            lambda row: passed[k, row],
            narrow_base(me),
        )
        return flip(chip, k, chips) * 2 + 1 - core

    stay.wait()
    pass_copy(0).start()
    refine_z(dims, pairs, mixed, rz, rz_lo, grid_ref, [from_direct(0, 0)])

    @pl.loop(1, chips)
    def _(k):
        out_copy(k).wait_recv()
        pass_copy(k).start()
        one = from_direct(0, k)
        pass_copy(k - 1).wait_recv()
        two = from_passed(1, k - 1)
        refine_z(dims, pairs, mixed, rz, rz_lo, grid_ref, [one, two])

    pass_copy(chips - 1).wait_recv()
    refine_z(dims, pairs, mixed, rz, rz_lo, grid_ref, [from_passed(0, chips - 1)])

    @pl.loop(1, chips)
    def _(k):
        out_copy(k).wait_send()

    @pl.loop(0, chips)
    def _(k):
        pass_copy(k).wait_send()


def relay(
    dims,
    points_ref, oy_ref, cy_ref, oz_ref, cz_ref, cx_ref,
    grid_ref, wx_ref,
    send, held, wy, rz, rz_lo, mixed,
    main_send, main_recv, pass_send, pass_recv, up_send, down_send, halo_recv, edge_send,
):
    n, comps, xl, ny, nz, jl, mz = dims
    chips = n // 2
    plane = chips // PLANES
    pairs, lanes = points_ref.shape[0], points_ref.shape[1]
    own = jl
    me = lax.axis_index("slab")
    chip, core = me // 2, me % 2
    partner = chip * 2 + 1 - core
    here, level = chip % plane, chip // plane
    middle = pl.ds(BELOW, own)
    rows_of_y = send.reshape(ny, pairs, lanes)

    barrier = pltpu.get_barrier_semaphore()

    @pl.loop(1, n)
    def _(k):
        pl.semaphore_signal(barrier, inc=1, device_id=((me + k) % n,), device_id_type=MESH)

    for p in range(pairs):
        send[pl.ds(p, ny, stride=pairs), :] = points_ref[p].T
    span_base = functools.partial(span_of, me, jl, ny)
    make_weights(dims, me, span_base, oy_ref, cy_ref, oz_ref, cz_ref, cx_ref, wx_ref, wy, rz, rz_lo)
    held[me, middle] = rows_of_y[pl.ds(chip * own, own)]

    pl.semaphore_wait(barrier, n - 1)

    def remote(src, dst, send_sem, recv_sem, device):
        return pltpu.make_async_remote_copy(
            src_ref=src, dst_ref=dst, send_sem=send_sem, recv_sem=recv_sem,
            device_id=(device,), device_id_type=MESH,
        )

    def main_copy(k):
        target = flip(chip, k, chips)
        return remote(
            rows_of_y.at[pl.ds(target * own, own)], held.at[me, middle],
            main_send.at[k], main_recv.at[k], target * 2 + core,
        )

    def main_arrival(k):
        source = flip(chip, k, chips) * 2 + core
        return remote(held.at[source, middle], held.at[source, middle], main_send.at[k], main_recv.at[k], partner)

    def pass_copy(k):
        source = flip(chip, k, chips) * 2 + core
        return remote(held.at[source, middle], held.at[source, middle], pass_send.at[k], pass_recv.at[k], partner)

    def pass_arrival(k):
        source = flip(chip, k, chips) * 2 + 1 - core
        return remote(held.at[source, middle], held.at[source, middle], pass_send.at[k], pass_recv.at[k], partner)

    def up_copy(k):
        source = flip(chip, k, chips) * 2 + core
        return remote(
            held.at[source, pl.ds(own, BELOW)], held.at[source, pl.ds(0, BELOW)],
            up_send.at[k], halo_recv.at[source], chip * 2 + 2,
        )

    def down_copy(k):
        source = flip(chip, k, chips) * 2 + core
        return remote(
            held.at[source, pl.ds(BELOW, ABOVE)], held.at[source, pl.ds(BELOW + own, ABOVE)],
            down_send.at[k], halo_recv.at[source], chip * 2 - 1,
        )

    has_up = here < plane - 1
    has_down = here > 0

    def edge_below(g):
        target = flip(level, g, PLANES) * plane
        copy = lambda: remote(
            rows_of_y.at[pl.ds(target * own - BELOW, BELOW)], held.at[me, pl.ds(0, BELOW)],
            edge_send.at[g], halo_recv.at[me], target * 2,
        )
        return (target > 0) & (target * 2 != me), copy

    def edge_above(g):
        target = flip(level, g, PLANES) * plane + plane - 1
        copy = lambda: remote(
            rows_of_y.at[pl.ds(target * own + own, ABOVE)], held.at[me, pl.ds(BELOW + own, ABOVE)],
            edge_send.at[PLANES + g], halo_recv.at[me], target * 2 + 1,
        )
        return (target < chips - 1) & (target * 2 + 1 != me), copy

    def send_edges(g):
        for edge in (edge_below, edge_above):
            needed, copy = edge(g)

            @pl.when(needed)
            def _():
                copy().start()

    def hand_on(k):
        pass_copy(k).start()

        @pl.when(has_up)
        def _():
            up_copy(k).start()

        @pl.when(has_down)
        def _():
            down_copy(k).start()

    @pl.loop(1, plane)
    def _(k):
        main_copy(k).start()

    send_edges(0)
    hand_on(0)

    for g in range(1, PLANES):

        @pl.loop(g * plane, (g + 1) * plane)
        def _(k):
            main_copy(k).start()

        send_edges(g)

    at_bottom = (here == 0) & (core == 0)
    at_top = (here == plane - 1) & (core == 1)

    @pl.when(at_bottom & (chip > 0))
    def _():
        held[me, 0:BELOW] = rows_of_y[pl.ds(chip * own - BELOW, BELOW)]

    @pl.when(at_top & (chip < chips - 1))
    def _():
        held[me, BELOW + own :] = rows_of_y[pl.ds(chip * own + own, ABOVE)]

    def await_halo(source):
        away = (source != me) | ((here != 0) & (core == 0)) | ((here != plane - 1) & (core == 1))

        @pl.when(away & (core == 0) & (chip > 0))
        def _():
            rows = held.at[source, pl.ds(0, BELOW)]
            remote(rows, rows, up_send.at[0], halo_recv.at[source], partner).wait_recv()

        @pl.when(away & (core == 1) & (chip < chips - 1))
        def _():
            rows = held.at[source, pl.ds(BELOW + own, ABOVE)]
            remote(rows, rows, up_send.at[0], halo_recv.at[source], partner).wait_recv()

    def refine(k):
        other = flip(chip, k, chips) * 2
        pass_arrival(k).wait_recv()
        for c in range(2):
            await_halo(other + c)
        for c in range(2):
            refine_y(jl, pairs, span_base, wy, mixed, c, lambda row: held[other + c, row], chip * own - BELOW)
        refine_z(dims, pairs, mixed, rz, rz_lo, grid_ref, [other, other + 1])

    @pl.loop(1, plane)
    def _(k):
        main_arrival(k).wait_recv()
        hand_on(k)

    @pl.loop(1, PLANES)
    def _(g):
        @pl.loop(0, plane)
        def _(r):
            main_arrival(g * plane + r).wait_recv()
            hand_on(g * plane + r)

        @pl.loop(0, plane)
        def _(r):
            refine((g - 1) * plane + r)

    @pl.loop(0, plane)
    def _(r):
        refine((PLANES - 1) * plane + r)

    @pl.loop(1, chips)
    def _(k):
        main_copy(k).wait_send()

    @pl.loop(0, chips)
    def _(k):
        pass_copy(k).wait_send()

        @pl.when(has_up)
        def _():
            up_copy(k).wait_send()

        @pl.when(has_down)
        def _():
            down_copy(k).wait_send()

    for g in range(PLANES):
        for edge in (edge_below, edge_above):
            needed, copy = edge(g)

            @pl.when(needed)
            def _():
                copy().wait_send()


def refine_x(rows, ox_ref, wx_ref, grid_ref, out_ref):
    comps = grid_ref.shape[0]
    start = pl.program_id(0) * rows

    @pl.loop(0, rows, unroll=4)
    def _(r):
        i = start + r
        first = ox_ref[i]
        weights = [wx_ref[k, i] for k in range(BAND)]
        for c in range(comps):
            acc = weights[0] * grid_ref[c, first]
            for k in range(1, BAND):
                acc = acc + weights[k] * grid_ref[c, first + k]
            out_ref[c, r] = acc


def solution(mesh):
    n = mesh.shape["slab"]
    vmem = pl.BlockSpec(memory_space=pltpu.VMEM)
    smem = pl.BlockSpec(memory_space=pltpu.SMEM)

    def body(points, offsets_x, coeffs_x, offsets_y, coeffs_y, offsets_z, coeffs_z):
        comps, xl, ny, nz = points.shape
        nx = xl * n
        mx, my, mz = offsets_x.shape[0], offsets_y.shape[0], offsets_z.shape[0]
        jl = my // n
        fold = 128 // nz
        pairs = comps * xl // fold
        lanes = fold * nz
        chips = n // 2
        cl = jl // 2
        wide, narrow = 2 * cl + REACH, cl + REACH
        slab = jnp.transpose(points, (0, 1, 3, 2)).reshape(pairs, lanes, ny)
        f32, bf16 = jnp.float32, jnp.bfloat16
        if jl >= ABOVE and chips % PLANES == 0:
            kernel, name = relay, "relay"
            buffers = [pltpu.VMEM((n, BELOW + jl + ABOVE, pairs, lanes), f32)]
            counts = [chips] * 6 + [n, 2 * PLANES]
        else:
            kernel, name = exchange, "exchange"
            buffers = [
                pltpu.VMEM((chips, wide, pairs, lanes), f32),
                pltpu.VMEM((chips, narrow, pairs, lanes), f32),
            ]
            counts = [chips] * 4
        grid, wx = pl.pallas_call(
            functools.partial(kernel, (n, comps, xl, ny, nz, jl, mz)),
            out_shape=(
                pltpu.VMEM((comps, nx, jl, mz), f32),
                jax.ShapeDtypeStruct((BAND, mx), f32),
            ),
            in_specs=[vmem, smem, smem, vmem, vmem, vmem],
            out_specs=(vmem, vmem),
            scratch_shapes=[
                pltpu.VMEM((ny * pairs, lanes), f32),
                *buffers,
                pltpu.VMEM((jl * SPAN, pairs, lanes), f32),
                pltpu.VMEM((2 * lanes, fold * mz), bf16),
                pltpu.VMEM((lanes, fold * mz), bf16),
                pltpu.VMEM((2 * pairs * jl, lanes), f32),
                *[pltpu.SemaphoreType.DMA((count,)) for count in counts],
            ],
            compiler_params=pltpu.CompilerParams(collective_id=0, has_side_effects=True),
            name=name,
        )(slab, offsets_y, coeffs_y, offsets_z.reshape(1, mz), coeffs_z, coeffs_x)
        steps = 8
        rows = mx // steps
        return pl.pallas_call(
            functools.partial(refine_x, rows),
            out_shape=jax.ShapeDtypeStruct((comps, mx, jl, mz), f32),
            grid=(steps,),
            in_specs=[smem, smem, vmem],
            out_specs=pl.BlockSpec((comps, rows, jl, mz), lambda s: (0, s, 0, 0)),
            name="refine_x",
        )(offsets_x, wx, pltpu.with_memory_space_constraint(grid, pltpu.VMEM))

    return jax.shard_map(
        body,
        mesh=mesh,
        in_specs=(P(None, "slab", None, None), P(), P(), P(), P(), P(), P()),
        out_specs=P(None, None, "slab", None),
        check_vma=False,
    )
```

```python
import functools

import jax
import jax.numpy as jnp
from jax import lax
from jax.experimental import pallas as pl
from jax.experimental.pallas import tpu as pltpu
from jax.sharding import PartitionSpec as P

MESH = pl.DeviceIdType.MESH
BAND = 4
REACH = BAND + 1
SPAN = BAND + 2
BELOW, ABOVE = 2, 3
PLANES = 4
GROUP = 8


def flip(a, k, chips):
    out = 0
    bit = 1
    while bit < chips:
        a_bit, k_bit = (a // bit) % 2, (k // bit) % 2
        out = out + (a_bit + k_bit - 2 * a_bit * k_bit) * bit
        bit *= 2
    return out


def span_of(me, jl, ny, j):
    return jnp.clip((me * jl + j) // 2 - 2, 0, ny - SPAN)


def make_weights(dims, me, span_base, oy_ref, cy_ref, oz_ref, cz_ref, cx_ref, wx_ref, wy, rz, rz_lo):
    n, comps, xl, ny, nz, jl, mz = dims
    pairs, lanes = wy.shape[1], wy.shape[2]
    fold = lanes // nz
    wx_ref[...] = cx_ref[...] / jnp.sum(cx_ref[...], axis=0, keepdims=True)
    wz = cz_ref[...] / jnp.sum(cz_ref[...], axis=0, keepdims=True)
    at = lax.broadcasted_iota(jnp.int32, (nz, mz), 0)
    first = jnp.broadcast_to(oz_ref[...], (nz, mz))
    band = jnp.zeros((nz, mz), jnp.float32)
    for k in range(BAND):
        band = band + jnp.where(at == first + k, jnp.broadcast_to(wz[k : k + 1], (nz, mz)), 0.0)
    high = band.astype(jnp.bfloat16)
    low = (band - high.astype(jnp.float32)).astype(jnp.bfloat16)
    rz[...] = jnp.zeros_like(rz)
    rz_lo[...] = jnp.zeros_like(rz_lo)
    for f in range(fold):
        rz[f * nz : (f + 1) * nz, f * mz : (f + 1) * mz] = high
        rz[lanes + f * nz : lanes + (f + 1) * nz, f * mz : (f + 1) * mz] = high
        rz_lo[f * nz : (f + 1) * nz, f * mz : (f + 1) * mz] = low
    for j in range(jl):
        coeffs = [jnp.full((pairs, lanes), cy_ref[k, me * jl + j]) for k in range(BAND)]
        total = coeffs[0] + coeffs[1] + coeffs[2] + coeffs[3]
        coeffs = [c / total for c in coeffs]
        skip = jnp.full((pairs, lanes), oy_ref[me * jl + j] - span_base(j))
        for m in range(SPAN):
            weight = jnp.zeros((pairs, lanes), jnp.float32)
            for k in range(max(0, m - SPAN + BAND), min(BAND, m + 1)):
                weight = jnp.where(skip == m - k, coeffs[k], weight)
            wy[j * SPAN + m] = weight


def refine_y(jl, pairs, span_base, wy, mixed, place, load, base):
    for j in range(jl):
        row = span_base(j) - base
        acc = wy[j * SPAN] * load(row)
        for m in range(1, SPAN):
            acc = acc + wy[j * SPAN + m] * load(row + m)
        mixed[pl.ds(place * pairs * jl + j, pairs, stride=jl), :] = acc


def refine_z(dims, pairs, mixed, rz, rz_lo, grid_ref, devices):
    n, comps, xl, ny, nz, jl, mz = dims
    fold = mixed.shape[1] // nz
    rows = pairs * jl * len(devices)
    x = mixed[:rows]
    hi = x.astype(jnp.bfloat16)
    lo = (x - hi.astype(jnp.float32)).astype(jnp.bfloat16)
    both = jnp.concatenate([hi, lo], axis=1)
    res = jnp.dot(both, rz[...], preferred_element_type=jnp.float32)
    res = res + jnp.dot(hi, rz_lo[...], preferred_element_type=jnp.float32)
    per = pairs // comps
    for q, device in enumerate(devices):
        for p in range(pairs):
            for f in range(fold):
                spot = (p // per, device * xl + (p % per) * fold + f)
                top = (q * pairs + p) * jl
                grid_ref[spot] = res[top : top + jl, f * mz : (f + 1) * mz]


def exchange(
    dims,
    points_ref, oy_ref, cy_ref, oz_ref, cz_ref, cx_ref,
    grid_ref, wx_ref,
    send, direct, passed, wy, rz, rz_lo, mixed,
    send_sem, recv_sem, pass_send_sem, pass_recv_sem,
):
    n, comps, xl, ny, nz, jl, mz = dims
    chips = n // 2
    pairs, lanes = points_ref.shape[0], points_ref.shape[1]
    cl = jl // 2
    wide, narrow = 2 * cl + REACH, cl + REACH
    me = lax.axis_index("slab")
    chip, core = me // 2, me % 2
    partner = chip * 2 + 1 - core

    def wide_base(c):
        return jnp.clip(c * 2 * cl - 2, 0, ny - wide)

    def narrow_base(d):
        return jnp.clip(d * cl - 2, 0, ny - narrow)

    span_base = functools.partial(span_of, me, jl, ny)

    rows_of_y = send.reshape(ny, pairs, lanes)

    barrier = pltpu.get_barrier_semaphore()
    pl.semaphore_signal(barrier, inc=1, device_id=(partner,), device_id_type=MESH)

    @pl.loop(1, chips)
    def _(k):
        other = flip(chip, k, chips) * 2 + core
        pl.semaphore_signal(barrier, inc=1, device_id=(other,), device_id_type=MESH)

    for p in range(pairs):
        send[pl.ds(p, ny, stride=pairs), :] = points_ref[p].T

    pl.semaphore_wait(barrier, chips)

    def out_copy(k):
        target = flip(chip, k, chips)
        return pltpu.make_async_remote_copy(
            src_ref=rows_of_y.at[pl.ds(wide_base(target), wide)],
            dst_ref=direct.at[k],
            send_sem=send_sem.at[k],
            recv_sem=recv_sem.at[k],
            device_id=(target * 2 + core,),
            device_id_type=MESH,
        )

    def pass_copy(k):
        skip = narrow_base(partner) - wide_base(chip)
        return pltpu.make_async_remote_copy(
            src_ref=direct.at[k, pl.ds(skip, narrow)],
            dst_ref=passed.at[k],
            send_sem=pass_send_sem.at[k],
            recv_sem=pass_recv_sem.at[k],
            device_id=(partner,),
            device_id_type=MESH,
        )

    @pl.loop(1, chips)
    def _(k):
        out_copy(k).start()

    own = pl.ds(wide_base(chip), wide)
    stay = pltpu.make_async_copy(rows_of_y.at[own], direct.at[0], recv_sem.at[0])
    stay.start()

    make_weights(dims, me, span_base, oy_ref, cy_ref, oz_ref, cz_ref, cx_ref, wx_ref, wy, rz, rz_lo)

    def from_direct(place, k):
        refine_y(
            jl, pairs, span_base, wy, mixed, place,
            lambda row: direct[k, row],
            wide_base(chip),
        )
        return flip(chip, k, chips) * 2 + core

    def from_passed(place, k):
        refine_y(
            jl, pairs, span_base, wy, mixed, place,
            lambda row: passed[k, row],
            narrow_base(me),
        )
        return flip(chip, k, chips) * 2 + 1 - core

    stay.wait()
    pass_copy(0).start()
    refine_z(dims, pairs, mixed, rz, rz_lo, grid_ref, [from_direct(0, 0)])

    @pl.loop(1, chips)
    def _(k):
        out_copy(k).wait_recv()
        pass_copy(k).start()
        one = from_direct(0, k)
        pass_copy(k - 1).wait_recv()
        two = from_passed(1, k - 1)
        refine_z(dims, pairs, mixed, rz, rz_lo, grid_ref, [one, two])

    pass_copy(chips - 1).wait_recv()
    refine_z(dims, pairs, mixed, rz, rz_lo, grid_ref, [from_passed(0, chips - 1)])

    @pl.loop(1, chips)
    def _(k):
        out_copy(k).wait_send()

    @pl.loop(0, chips)
    def _(k):
        pass_copy(k).wait_send()


def relay(
    dims,
    points_ref, oy_ref, cy_ref, oz_ref, cz_ref, cx_ref,
    grid_ref, wx_ref,
    send, held, wy, rz, rz_lo, mixed,
    main_send, main_recv, pass_send, pass_recv, up_send, down_send, halo_recv, edge_send,
):
    n, comps, xl, ny, nz, jl, mz = dims
    chips = n // 2
    plane = chips // PLANES
    pairs, lanes = points_ref.shape[0], points_ref.shape[1]
    own = jl
    me = lax.axis_index("slab")
    chip, core = me // 2, me % 2
    partner = chip * 2 + 1 - core
    here, level = chip % plane, chip // plane
    middle = pl.ds(BELOW, own)
    rows_of_y = send.reshape(ny, pairs, lanes)

    barrier = pltpu.get_barrier_semaphore()

    @pl.loop(1, n)
    def _(k):
        pl.semaphore_signal(barrier, inc=1, device_id=((me + k) % n,), device_id_type=MESH)

    for p in range(pairs):
        send[pl.ds(p, ny, stride=pairs), :] = points_ref[p].T
    span_base = functools.partial(span_of, me, jl, ny)
    make_weights(dims, me, span_base, oy_ref, cy_ref, oz_ref, cz_ref, cx_ref, wx_ref, wy, rz, rz_lo)
    held[me, middle] = rows_of_y[pl.ds(chip * own, own)]

    pl.semaphore_wait(barrier, n - 1)

    def remote(src, dst, send_sem, recv_sem, device):
        return pltpu.make_async_remote_copy(
            src_ref=src, dst_ref=dst, send_sem=send_sem, recv_sem=recv_sem,
            device_id=(device,), device_id_type=MESH,
        )

    def main_copy(k):
        target = flip(chip, k, chips)
        return remote(
            rows_of_y.at[pl.ds(target * own, own)], held.at[me, middle],
            main_send.at[k], main_recv.at[k], target * 2 + core,
        )

    def main_arrival(k):
        source = flip(chip, k, chips) * 2 + core
        return remote(held.at[source, middle], held.at[source, middle], main_send.at[k], main_recv.at[k], partner)

    def pass_copy(k):
        source = flip(chip, k, chips) * 2 + core
        return remote(held.at[source, middle], held.at[source, middle], pass_send.at[k], pass_recv.at[k], partner)

    def pass_arrival(k):
        source = flip(chip, k, chips) * 2 + 1 - core
        return remote(held.at[source, middle], held.at[source, middle], pass_send.at[k], pass_recv.at[k], partner)

    def up_copy(k):
        source = flip(chip, k, chips) * 2 + core
        return remote(
            held.at[source, pl.ds(own, BELOW)], held.at[source, pl.ds(0, BELOW)],
            up_send.at[k], halo_recv.at[source], chip * 2 + 2,
        )

    def down_copy(k):
        source = flip(chip, k, chips) * 2 + core
        return remote(
            held.at[source, pl.ds(BELOW, ABOVE)], held.at[source, pl.ds(BELOW + own, ABOVE)],
            down_send.at[k], halo_recv.at[source], chip * 2 - 1,
        )

    has_up = here < plane - 1
    has_down = here > 0

    def edge_below(g):
        target = flip(level, g, PLANES) * plane
        copy = lambda: remote(
            rows_of_y.at[pl.ds(target * own - BELOW, BELOW)], held.at[me, pl.ds(0, BELOW)],
            edge_send.at[g], halo_recv.at[me], target * 2,
        )
        return (target > 0) & (target * 2 != me), copy

    def edge_above(g):
        target = flip(level, g, PLANES) * plane + plane - 1
        copy = lambda: remote(
            rows_of_y.at[pl.ds(target * own + own, ABOVE)], held.at[me, pl.ds(BELOW + own, ABOVE)],
            edge_send.at[PLANES + g], halo_recv.at[me], target * 2 + 1,
        )
        return (target < chips - 1) & (target * 2 + 1 != me), copy

    def send_edges(g):
        for edge in (edge_below, edge_above):
            needed, copy = edge(g)

            @pl.when(needed)
            def _():
                copy().start()

    def hand_on(k):
        pass_copy(k).start()

        @pl.when(has_up)
        def _():
            up_copy(k).start()

        @pl.when(has_down)
        def _():
            down_copy(k).start()

    @pl.loop(1, plane)
    def _(k):
        main_copy(k).start()

    send_edges(0)
    hand_on(0)

    for g in range(1, PLANES):

        @pl.loop(g * plane, (g + 1) * plane)
        def _(k):
            main_copy(k).start()

        send_edges(g)

    at_bottom = (here == 0) & (core == 0)
    at_top = (here == plane - 1) & (core == 1)

    @pl.when(at_bottom & (chip > 0))
    def _():
        held[me, 0:BELOW] = rows_of_y[pl.ds(chip * own - BELOW, BELOW)]

    @pl.when(at_top & (chip < chips - 1))
    def _():
        held[me, BELOW + own :] = rows_of_y[pl.ds(chip * own + own, ABOVE)]

    def await_halo(source):
        away = (source != me) | ((here != 0) & (core == 0)) | ((here != plane - 1) & (core == 1))

        @pl.when(away & (core == 0) & (chip > 0))
        def _():
            rows = held.at[source, pl.ds(0, BELOW)]
            remote(rows, rows, up_send.at[0], halo_recv.at[source], partner).wait_recv()

        @pl.when(away & (core == 1) & (chip < chips - 1))
        def _():
            rows = held.at[source, pl.ds(BELOW + own, ABOVE)]
            remote(rows, rows, up_send.at[0], halo_recv.at[source], partner).wait_recv()

    def refine(k):
        others = [flip(chip, k + i, chips) * 2 for i in range(2)]
        for i in range(2):
            pass_arrival(k + i).wait_recv()
        devices = [other + c for other in others for c in range(2)]
        for device in devices:
            await_halo(device)
        for j in range(jl):
            row = span_base(j) - (chip * own - BELOW)
            sums = [None] * len(devices)
            for m in range(SPAN):
                weight = wy[j * SPAN + m]
                for i, device in enumerate(devices):
                    term = weight * held[device, row + m]
                    sums[i] = term if m == 0 else sums[i] + term
            for i, total in enumerate(sums):
                mixed[pl.ds(i * pairs * jl + j, pairs, stride=jl), :] = total
        refine_z(dims, pairs, mixed, rz, rz_lo, grid_ref, devices)

    def take(k):
        main_arrival(k).wait_recv()
        hand_on(k)

    @pl.loop(1, plane)
    def _(k):
        take(k)

    @pl.loop(plane // 2, chips // 2)
    def _(h):
        take(2 * h)
        take(2 * h + 1)
        refine(2 * h - plane)

    @pl.loop((chips - plane) // 2, chips // 2)
    def _(h):
        refine(2 * h)

    @pl.loop(1, chips)
    def _(k):
        main_copy(k).wait_send()

    @pl.loop(0, chips)
    def _(k):
        pass_copy(k).wait_send()

        @pl.when(has_up)
        def _():
            up_copy(k).wait_send()

        @pl.when(has_down)
        def _():
            down_copy(k).wait_send()

    for g in range(PLANES):
        for edge in (edge_below, edge_above):
            needed, copy = edge(g)

            @pl.when(needed)
            def _():
                copy().wait_send()


def refine_x(steps, ox_ref, wx_ref, grid_ref, out_ref, block, sems):
    comps, mx = block.shape[0], block.shape[1]
    rows = mx // steps

    def put(s):
        part = pl.ds(pl.multiple_of(s * rows, rows), rows)
        return pltpu.make_async_copy(block.at[:, part], out_ref.at[:, part], sems.at[s])

    @pl.loop(0, steps)
    def _(s):
        @pl.loop(0, rows // GROUP)
        def _(g):
            done = []
            for q in range(GROUP):
                i = s * rows + g * GROUP + q
                first = ox_ref[i]
                weights = [wx_ref[k, i] for k in range(BAND)]
                for c in range(comps):
                    acc = weights[0] * grid_ref[c, first]
                    for k in range(1, BAND):
                        acc = acc + weights[k] * grid_ref[c, first + k]
                    done.append((c, i, acc))
            for c, i, acc in done:
                block[c, i] = acc

        put(s).start()

    @pl.loop(0, steps)
    def _(s):
        put(s).wait()


def solution(mesh):
    n = mesh.shape["slab"]
    vmem = pl.BlockSpec(memory_space=pltpu.VMEM)
    smem = pl.BlockSpec(memory_space=pltpu.SMEM)

    def body(points, offsets_x, coeffs_x, offsets_y, coeffs_y, offsets_z, coeffs_z):
        comps, xl, ny, nz = points.shape
        nx = xl * n
        mx, my, mz = offsets_x.shape[0], offsets_y.shape[0], offsets_z.shape[0]
        jl = my // n
        fold = 128 // nz
        pairs = comps * xl // fold
        lanes = fold * nz
        chips = n // 2
        cl = jl // 2
        wide, narrow = 2 * cl + REACH, cl + REACH
        slab = jnp.transpose(points, (0, 1, 3, 2)).reshape(pairs, lanes, ny)
        f32, bf16 = jnp.float32, jnp.bfloat16
        if jl >= ABOVE and chips % PLANES == 0:
            kernel, name = relay, "relay"
            buffers = [pltpu.VMEM((n, BELOW + jl + ABOVE, pairs, lanes), f32)]
            counts = [chips] * 6 + [n, 2 * PLANES]
        else:
            kernel, name = exchange, "exchange"
            buffers = [
                pltpu.VMEM((chips, wide, pairs, lanes), f32),
                pltpu.VMEM((chips, narrow, pairs, lanes), f32),
            ]
            counts = [chips] * 4
        grid, wx = pl.pallas_call(
            functools.partial(kernel, (n, comps, xl, ny, nz, jl, mz)),
            out_shape=(
                pltpu.VMEM((comps, nx, jl, mz), f32),
                jax.ShapeDtypeStruct((BAND, mx), f32),
            ),
            in_specs=[vmem, smem, smem, vmem, vmem, vmem],
            out_specs=(vmem, vmem),
            scratch_shapes=[
                pltpu.VMEM((ny * pairs, lanes), f32),
                *buffers,
                pltpu.VMEM((jl * SPAN, pairs, lanes), f32),
                pltpu.VMEM((2 * lanes, fold * mz), bf16),
                pltpu.VMEM((lanes, fold * mz), bf16),
                pltpu.VMEM((4 * pairs * jl, lanes), f32),
                *[pltpu.SemaphoreType.DMA((count,)) for count in counts],
            ],
            compiler_params=pltpu.CompilerParams(collective_id=0, has_side_effects=True),
            name=name,
        )(slab, offsets_y, coeffs_y, offsets_z.reshape(1, mz), coeffs_z, coeffs_x)
        steps = 8
        return pl.pallas_call(
            functools.partial(refine_x, steps),
            out_shape=jax.ShapeDtypeStruct((comps, mx, jl, mz), f32),
            in_specs=[smem, smem, vmem],
            out_specs=pl.BlockSpec(memory_space=pltpu.HBM),
            scratch_shapes=[
                pltpu.VMEM((comps, mx, jl, mz), f32),
                pltpu.SemaphoreType.DMA((steps,)),
            ],
            name="refine_x",
        )(offsets_x, wx, pltpu.with_memory_space_constraint(grid, pltpu.VMEM))

    return jax.shard_map(
        body,
        mesh=mesh,
        in_specs=(P(None, "slab", None, None), P(), P(), P(), P(), P(), P()),
        out_specs=P(None, None, "slab", None),
        check_vma=False,
    )
```

```python
import functools

import jax
import jax.numpy as jnp
from jax import lax
from jax.experimental import pallas as pl
from jax.experimental.pallas import tpu as pltpu
from jax.sharding import PartitionSpec as P

MESH = pl.DeviceIdType.MESH
BAND = 4
REACH = BAND + 1
SPAN = BAND + 2
BELOW, ABOVE = 2, 3
PLANES = 4
GROUP = 8


def flip(a, k, chips):
    out = 0
    bit = 1
    while bit < chips:
        a_bit, k_bit = (a // bit) % 2, (k // bit) % 2
        out = out + (a_bit + k_bit - 2 * a_bit * k_bit) * bit
        bit *= 2
    return out


def span_of(me, jl, ny, j):
    return jnp.clip((me * jl + j) // 2 - 2, 0, ny - SPAN)


def make_weights(dims, me, span_base, oy_ref, cy_ref, oz_ref, cz_ref, cx_ref, wx_ref, wy, rz, rz_lo):
    n, comps, xl, ny, nz, jl, mz = dims
    pairs, lanes = wy.shape[1], wy.shape[2]
    fold = lanes // nz
    wx_ref[...] = cx_ref[...] / jnp.sum(cx_ref[...], axis=0, keepdims=True)
    wz = cz_ref[...] / jnp.sum(cz_ref[...], axis=0, keepdims=True)
    at = lax.broadcasted_iota(jnp.int32, (nz, mz), 0)
    first = jnp.broadcast_to(oz_ref[...], (nz, mz))
    band = jnp.zeros((nz, mz), jnp.float32)
    for k in range(BAND):
        band = band + jnp.where(at == first + k, jnp.broadcast_to(wz[k : k + 1], (nz, mz)), 0.0)
    high = band.astype(jnp.bfloat16)
    low = (band - high.astype(jnp.float32)).astype(jnp.bfloat16)
    rz[...] = jnp.zeros_like(rz)
    rz_lo[...] = jnp.zeros_like(rz_lo)
    for f in range(fold):
        rz[f * nz : (f + 1) * nz, f * mz : (f + 1) * mz] = high
        rz[lanes + f * nz : lanes + (f + 1) * nz, f * mz : (f + 1) * mz] = high
        rz_lo[f * nz : (f + 1) * nz, f * mz : (f + 1) * mz] = low
    for j in range(jl):
        coeffs = [jnp.full((pairs, lanes), cy_ref[k, me * jl + j]) for k in range(BAND)]
        total = coeffs[0] + coeffs[1] + coeffs[2] + coeffs[3]
        coeffs = [c / total for c in coeffs]
        skip = jnp.full((pairs, lanes), oy_ref[me * jl + j] - span_base(j))
        for m in range(SPAN):
            weight = jnp.zeros((pairs, lanes), jnp.float32)
            for k in range(max(0, m - SPAN + BAND), min(BAND, m + 1)):
                weight = jnp.where(skip == m - k, coeffs[k], weight)
            wy[j * SPAN + m] = weight


def refine_y(jl, pairs, span_base, wy, mixed, place, load, base):
    for j in range(jl):
        row = span_base(j) - base
        acc = wy[j * SPAN] * load(row)
        for m in range(1, SPAN):
            acc = acc + wy[j * SPAN + m] * load(row + m)
        mixed[pl.ds(place * pairs * jl + j, pairs, stride=jl), :] = acc


def refine_z(dims, pairs, mixed, rz, rz_lo, grid_ref, devices):
    n, comps, xl, ny, nz, jl, mz = dims
    fold = mixed.shape[1] // nz
    rows = pairs * jl * len(devices)
    x = mixed[:rows]
    hi = x.astype(jnp.bfloat16)
    lo = (x - hi.astype(jnp.float32)).astype(jnp.bfloat16)
    both = jnp.concatenate([hi, lo], axis=1)
    res = jnp.dot(both, rz[...], preferred_element_type=jnp.float32)
    res = res + jnp.dot(hi, rz_lo[...], preferred_element_type=jnp.float32)
    per = pairs // comps
    for q, device in enumerate(devices):
        for p in range(pairs):
            for f in range(fold):
                spot = (p // per, device * xl + (p % per) * fold + f)
                top = (q * pairs + p) * jl
                grid_ref[spot] = res[top : top + jl, f * mz : (f + 1) * mz]


def exchange(
    dims,
    points_ref, oy_ref, cy_ref, oz_ref, cz_ref, cx_ref,
    grid_ref, wx_ref,
    send, direct, passed, wy, rz, rz_lo, mixed,
    send_sem, recv_sem, pass_send_sem, pass_recv_sem,
):
    n, comps, xl, ny, nz, jl, mz = dims
    chips = n // 2
    pairs, lanes = points_ref.shape[0], points_ref.shape[1]
    cl = jl // 2
    wide, narrow = 2 * cl + REACH, cl + REACH
    me = lax.axis_index("slab")
    chip, core = me // 2, me % 2
    partner = chip * 2 + 1 - core

    def wide_base(c):
        return jnp.clip(c * 2 * cl - 2, 0, ny - wide)

    def narrow_base(d):
        return jnp.clip(d * cl - 2, 0, ny - narrow)

    span_base = functools.partial(span_of, me, jl, ny)

    rows_of_y = send.reshape(ny, pairs, lanes)

    barrier = pltpu.get_barrier_semaphore()
    pl.semaphore_signal(barrier, inc=1, device_id=(partner,), device_id_type=MESH)

    @pl.loop(1, chips)
    def _(k):
        other = flip(chip, k, chips) * 2 + core
        pl.semaphore_signal(barrier, inc=1, device_id=(other,), device_id_type=MESH)

    for p in range(pairs):
        send[pl.ds(p, ny, stride=pairs), :] = points_ref[p].T

    pl.semaphore_wait(barrier, chips)

    def out_copy(k):
        target = flip(chip, k, chips)
        return pltpu.make_async_remote_copy(
            src_ref=rows_of_y.at[pl.ds(wide_base(target), wide)],
            dst_ref=direct.at[k],
            send_sem=send_sem.at[k],
            recv_sem=recv_sem.at[k],
            device_id=(target * 2 + core,),
            device_id_type=MESH,
        )

    def pass_copy(k):
        skip = narrow_base(partner) - wide_base(chip)
        return pltpu.make_async_remote_copy(
            src_ref=direct.at[k, pl.ds(skip, narrow)],
            dst_ref=passed.at[k],
            send_sem=pass_send_sem.at[k],
            recv_sem=pass_recv_sem.at[k],
            device_id=(partner,),
            device_id_type=MESH,
        )

    @pl.loop(1, chips)
    def _(k):
        out_copy(k).start()

    own = pl.ds(wide_base(chip), wide)
    stay = pltpu.make_async_copy(rows_of_y.at[own], direct.at[0], recv_sem.at[0])
    stay.start()

    make_weights(dims, me, span_base, oy_ref, cy_ref, oz_ref, cz_ref, cx_ref, wx_ref, wy, rz, rz_lo)

    def from_direct(place, k):
        refine_y(
            jl, pairs, span_base, wy, mixed, place,
            lambda row: direct[k, row],
            wide_base(chip),
        )
        return flip(chip, k, chips) * 2 + core

    def from_passed(place, k):
        refine_y(
            jl, pairs, span_base, wy, mixed, place,
            lambda row: passed[k, row],
            narrow_base(me),
        )
        return flip(chip, k, chips) * 2 + 1 - core

    stay.wait()
    pass_copy(0).start()
    refine_z(dims, pairs, mixed, rz, rz_lo, grid_ref, [from_direct(0, 0)])

    @pl.loop(1, chips)
    def _(k):
        out_copy(k).wait_recv()
        pass_copy(k).start()
        one = from_direct(0, k)
        pass_copy(k - 1).wait_recv()
        two = from_passed(1, k - 1)
        refine_z(dims, pairs, mixed, rz, rz_lo, grid_ref, [one, two])

    pass_copy(chips - 1).wait_recv()
    refine_z(dims, pairs, mixed, rz, rz_lo, grid_ref, [from_passed(0, chips - 1)])

    @pl.loop(1, chips)
    def _(k):
        out_copy(k).wait_send()

    @pl.loop(0, chips)
    def _(k):
        pass_copy(k).wait_send()


def relay(
    dims,
    points_ref, oy_ref, cy_ref, oz_ref, cz_ref, cx_ref,
    grid_ref, wx_ref,
    send, held, wy, rz, rz_lo, mixed,
    main_send, main_recv, pass_send, pass_recv, up_send, down_send, halo_recv, edge_send,
):
    n, comps, xl, ny, nz, jl, mz = dims
    chips = n // 2
    plane = chips // PLANES
    pairs, lanes = points_ref.shape[0], points_ref.shape[1]
    own = jl
    me = lax.axis_index("slab")
    chip, core = me // 2, me % 2
    partner = chip * 2 + 1 - core
    here, level = chip % plane, chip // plane
    middle = pl.ds(BELOW, own)
    rows_of_y = send.reshape(ny, pairs, lanes)

    barrier = pltpu.get_barrier_semaphore()

    @pl.loop(1, n)
    def _(k):
        pl.semaphore_signal(barrier, inc=1, device_id=((me + k) % n,), device_id_type=MESH)

    for p in range(pairs):
        send[pl.ds(p, ny, stride=pairs), :] = points_ref[p].T
    span_base = functools.partial(span_of, me, jl, ny)
    make_weights(dims, me, span_base, oy_ref, cy_ref, oz_ref, cz_ref, cx_ref, wx_ref, wy, rz, rz_lo)
    held[me, middle] = rows_of_y[pl.ds(chip * own, own)]

    pl.semaphore_wait(barrier, n - 1)

    def remote(src, dst, send_sem, recv_sem, device):
        return pltpu.make_async_remote_copy(
            src_ref=src, dst_ref=dst, send_sem=send_sem, recv_sem=recv_sem,
            device_id=(device,), device_id_type=MESH,
        )

    def main_copy(k):
        target = flip(chip, k, chips)
        return remote(
            rows_of_y.at[pl.ds(target * own, own)], held.at[me, middle],
            main_send.at[k], main_recv.at[k], target * 2 + core,
        )

    def main_arrival(k):
        source = flip(chip, k, chips) * 2 + core
        return remote(held.at[source, middle], held.at[source, middle], main_send.at[k], main_recv.at[k], partner)

    def pass_copy(k):
        source = flip(chip, k, chips) * 2 + core
        return remote(held.at[source, middle], held.at[source, middle], pass_send.at[k], pass_recv.at[k], partner)

    def pass_arrival(k):
        source = flip(chip, k, chips) * 2 + 1 - core
        return remote(held.at[source, middle], held.at[source, middle], pass_send.at[k], pass_recv.at[k], partner)

    def up_copy(k):
        source = flip(chip, k, chips) * 2 + core
        return remote(
            held.at[source, pl.ds(own, BELOW)], held.at[source, pl.ds(0, BELOW)],
            up_send.at[k], halo_recv.at[source], chip * 2 + 2,
        )

    def down_copy(k):
        source = flip(chip, k, chips) * 2 + core
        return remote(
            held.at[source, pl.ds(BELOW, ABOVE)], held.at[source, pl.ds(BELOW + own, ABOVE)],
            down_send.at[k], halo_recv.at[source], chip * 2 - 1,
        )

    has_up = here < plane - 1
    has_down = here > 0

    def edge_below(g):
        target = flip(level, g, PLANES) * plane
        copy = lambda: remote(
            rows_of_y.at[pl.ds(target * own - BELOW, BELOW)], held.at[me, pl.ds(0, BELOW)],
            edge_send.at[g], halo_recv.at[me], target * 2,
        )
        return (target > 0) & (target * 2 != me), copy

    def edge_above(g):
        target = flip(level, g, PLANES) * plane + plane - 1
        copy = lambda: remote(
            rows_of_y.at[pl.ds(target * own + own, ABOVE)], held.at[me, pl.ds(BELOW + own, ABOVE)],
            edge_send.at[PLANES + g], halo_recv.at[me], target * 2 + 1,
        )
        return (target < chips - 1) & (target * 2 + 1 != me), copy

    def send_edges(g):
        for edge in (edge_below, edge_above):
            needed, copy = edge(g)

            @pl.when(needed)
            def _():
                copy().start()

    def hand_on(k):
        pass_copy(k).start()

        @pl.when(has_up)
        def _():
            up_copy(k).start()

        @pl.when(has_down)
        def _():
            down_copy(k).start()

    @pl.loop(1, plane)
    def _(k):
        main_copy(k).start()

    send_edges(0)
    hand_on(0)

    for g in range(1, PLANES):

        @pl.loop(g * plane, (g + 1) * plane)
        def _(k):
            main_copy(k).start()

        send_edges(g)

    at_bottom = (here == 0) & (core == 0)
    at_top = (here == plane - 1) & (core == 1)

    @pl.when(at_bottom & (chip > 0))
    def _():
        held[me, 0:BELOW] = rows_of_y[pl.ds(chip * own - BELOW, BELOW)]

    @pl.when(at_top & (chip < chips - 1))
    def _():
        held[me, BELOW + own :] = rows_of_y[pl.ds(chip * own + own, ABOVE)]

    def await_halo(source):
        away = (source != me) | ((here != 0) & (core == 0)) | ((here != plane - 1) & (core == 1))

        @pl.when(away & (core == 0) & (chip > 0))
        def _():
            rows = held.at[source, pl.ds(0, BELOW)]
            remote(rows, rows, up_send.at[0], halo_recv.at[source], partner).wait_recv()

        @pl.when(away & (core == 1) & (chip < chips - 1))
        def _():
            rows = held.at[source, pl.ds(BELOW + own, ABOVE)]
            remote(rows, rows, up_send.at[0], halo_recv.at[source], partner).wait_recv()

    def refine(k):
        others = [flip(chip, k + i, chips) * 2 for i in range(2)]
        for i in range(2):
            pass_arrival(k + i).wait_recv()
        devices = [other + c for other in others for c in range(2)]
        for device in devices:
            await_halo(device)
        for j in range(jl):
            row = span_base(j) - (chip * own - BELOW)
            sums = [None] * len(devices)
            for m in range(SPAN):
                weight = wy[j * SPAN + m]
                for i, device in enumerate(devices):
                    term = weight * held[device, row + m]
                    sums[i] = term if m == 0 else sums[i] + term
            for i, total in enumerate(sums):
                mixed[pl.ds(i * pairs * jl + j, pairs, stride=jl), :] = total
        refine_z(dims, pairs, mixed, rz, rz_lo, grid_ref, devices)

    def take(k):
        main_arrival(k).wait_recv()
        hand_on(k)

    @pl.loop(1, plane)
    def _(k):
        take(k)

    @pl.loop(1, PLANES)
    def _(g):
        @pl.loop(0, plane)
        def _(r):
            take(g * plane + r)

        @pl.loop(0, plane // 2)
        def _(h):
            refine((g - 1) * plane + 2 * h)

    @pl.loop((chips - plane) // 2, chips // 2)
    def _(h):
        refine(2 * h)

    @pl.loop(1, chips)
    def _(k):
        main_copy(k).wait_send()

    @pl.loop(0, chips)
    def _(k):
        pass_copy(k).wait_send()

        @pl.when(has_up)
        def _():
            up_copy(k).wait_send()

        @pl.when(has_down)
        def _():
            down_copy(k).wait_send()

    for g in range(PLANES):
        for edge in (edge_below, edge_above):
            needed, copy = edge(g)

            @pl.when(needed)
            def _():
                copy().wait_send()


def refine_x(steps, ox_ref, wx_ref, grid_ref, out_ref, block, sems):
    comps, mx = block.shape[0], block.shape[1]
    rows = mx // steps

    def put(s):
        part = pl.ds(pl.multiple_of(s * rows, rows), rows)
        return pltpu.make_async_copy(block.at[:, part], out_ref.at[:, part], sems.at[s])

    @pl.loop(0, steps)
    def _(s):
        @pl.loop(0, rows // GROUP)
        def _(g):
            done = []
            for q in range(GROUP):
                i = s * rows + g * GROUP + q
                first = ox_ref[i]
                weights = [wx_ref[k, i] for k in range(BAND)]
                for c in range(comps):
                    acc = weights[0] * grid_ref[c, first]
                    for k in range(1, BAND):
                        acc = acc + weights[k] * grid_ref[c, first + k]
                    done.append((c, i, acc))
            for c, i, acc in done:
                block[c, i] = acc

        put(s).start()

    @pl.loop(0, steps)
    def _(s):
        put(s).wait()


def solution(mesh):
    n = mesh.shape["slab"]
    vmem = pl.BlockSpec(memory_space=pltpu.VMEM)
    smem = pl.BlockSpec(memory_space=pltpu.SMEM)

    def body(points, offsets_x, coeffs_x, offsets_y, coeffs_y, offsets_z, coeffs_z):
        comps, xl, ny, nz = points.shape
        nx = xl * n
        mx, my, mz = offsets_x.shape[0], offsets_y.shape[0], offsets_z.shape[0]
        jl = my // n
        fold = 128 // nz
        pairs = comps * xl // fold
        lanes = fold * nz
        chips = n // 2
        cl = jl // 2
        wide, narrow = 2 * cl + REACH, cl + REACH
        slab = jnp.transpose(points, (0, 1, 3, 2)).reshape(pairs, lanes, ny)
        f32, bf16 = jnp.float32, jnp.bfloat16
        if jl >= ABOVE and chips % PLANES == 0:
            kernel, name = relay, "relay"
            buffers = [pltpu.VMEM((n, BELOW + jl + ABOVE, pairs, lanes), f32)]
            counts = [chips] * 6 + [n, 2 * PLANES]
        else:
            kernel, name = exchange, "exchange"
            buffers = [
                pltpu.VMEM((chips, wide, pairs, lanes), f32),
                pltpu.VMEM((chips, narrow, pairs, lanes), f32),
            ]
            counts = [chips] * 4
        grid, wx = pl.pallas_call(
            functools.partial(kernel, (n, comps, xl, ny, nz, jl, mz)),
            out_shape=(
                pltpu.VMEM((comps, nx, jl, mz), f32),
                jax.ShapeDtypeStruct((BAND, mx), f32),
            ),
            in_specs=[vmem, smem, smem, vmem, vmem, vmem],
            out_specs=(vmem, vmem),
            scratch_shapes=[
                pltpu.VMEM((ny * pairs, lanes), f32),
                *buffers,
                pltpu.VMEM((jl * SPAN, pairs, lanes), f32),
                pltpu.VMEM((2 * lanes, fold * mz), bf16),
                pltpu.VMEM((lanes, fold * mz), bf16),
                pltpu.VMEM((4 * pairs * jl, lanes), f32),
                *[pltpu.SemaphoreType.DMA((count,)) for count in counts],
            ],
            compiler_params=pltpu.CompilerParams(collective_id=0, has_side_effects=True),
            name=name,
        )(slab, offsets_y, coeffs_y, offsets_z.reshape(1, mz), coeffs_z, coeffs_x)
        steps = 8
        return pl.pallas_call(
            functools.partial(refine_x, steps),
            out_shape=jax.ShapeDtypeStruct((comps, mx, jl, mz), f32),
            in_specs=[smem, smem, vmem],
            out_specs=pl.BlockSpec(memory_space=pltpu.HBM),
            scratch_shapes=[
                pltpu.VMEM((comps, mx, jl, mz), f32),
                pltpu.SemaphoreType.DMA((steps,)),
            ],
            name="refine_x",
        )(offsets_x, wx, pltpu.with_memory_space_constraint(grid, pltpu.VMEM))

    return jax.shard_map(
        body,
        mesh=mesh,
        in_specs=(P(None, "slab", None, None), P(), P(), P(), P(), P(), P()),
        out_specs=P(None, None, "slab", None),
        check_vma=False,
    )
```
